1024 devices in a mesh: cuts: 16 (over z_hi, x, core), stem: 64 (over y, z_lo).
Axes of the slice: x: 4, y: 8, z: 16 (z_hi: 2, z_lo: 8; z = z_hi * 8 + z_lo), core: 2. Of those that a mesh axis runs over, the one named last changes fastest.
Arguments:
- stems: bfloat16 [16, 64, 128, 2, 512], P('cuts', 'stem'), may hold values from -6 to 6
- branches: bfloat16 [2, 2, 2, 512, 512], replicated, may hold values from -0.1875 to 0.1875
- closing: bfloat16 [2, 2, 512, 256], replicated, may hold values from -0.046875 to 0.046875
- slice_values: int32 [16, 3], P('cuts'), may hold values from 0 to 1
- mode_perms: int32 [3, 9], replicated, may hold values from 0 to 8, each once within a row
- owner_map: int32 [16], replicated, may hold values from 0 to 15, each once
Outputs:
- open_amplitudes: float32 [64, 16, 2, 16, 128], P('stem', 'cuts')
The draws below stay inside these ranges and needn't reach their ends.
Inputs may be any that keep to these rules, and one draw needn't show every extreme that they name: `mode_perms`: each row is a permutation of the 9 modes. `owner_map`: a permutation of the owner indices.
All inputs are finite; a program needn't handle non-finite values.
Results may differ from the reference program's by a relative error of at most 0.017.
Values may be sent and summed in bfloat16 or wider, within the bound.
A program may use at most 32 MiB of HBM per device.

```python
import jax
import jax.numpy as jnp
from jax import lax

MODES = 9
WIDTH = 512
HALF = 256
ROWS = 128
VARIANTS = 2
SLICES = 16
PIECE = 16
N_CUTS = 16
N_STEM = 64


def touch_ends(array, rng, least, top_value):
    spot = [jax.random.randint(jax.random.fold_in(rng, axis), (), 0, length) for axis, length in enumerate(array.shape)]
    longest = array.shape.index(max(array.shape))
    neighbour = spot[:longest] + [(spot[longest] + 1) % array.shape[longest]] + spot[longest + 1:]
    return array.at[tuple(spot)].set(least).at[tuple(neighbour)].set(top_value)


def steps_of(rng, extent, pieces, smallest, high):
    def one(dim, blocks):
        heights = jax.random.uniform(jax.random.fold_in(jax.random.fold_in(rng, 6), dim), (blocks,), jnp.float32, smallest / len(pieces), high / len(pieces))
        return jnp.repeat(jnp.exp(heights), extent[dim] // blocks).reshape((-1,) + (1,) * (len(extent) - dim - 1))

    loudness = one(*pieces[0])
    for cut in pieces[1:]:
        loudness = loudness * one(*cut)
    return loudness


def centred(key, shape, spread, bound, shards=(), held_as=jnp.bfloat16):
    values = spread * jax.random.normal(key, shape, jnp.float32)
    if shards:
        values = values * steps_of(key, shape, shards, -0.22, 0.18)
    return jnp.clip(values, -bound, bound).astype(held_as)


def setup_inputs(seed: int = 0) -> dict:
    key_list = jax.random.split(jax.random.key(seed), 7)
    stems = centred(key_list[0], (SLICES, N_STEM, ROWS, 2, WIDTH), 1.0, 6.0, ((0, 16), (1, 64)))
    branches = centred(key_list[1], (2, VARIANTS, 2, WIDTH, WIDTH), (2 * WIDTH) ** -0.5, 0.1875)
    closing = centred(key_list[2], (VARIANTS, 2, WIDTH, HALF), (2 * WIDTH * N_CUTS) ** -0.5, 0.046875)
    slice_values = touch_ends(jax.random.randint(key_list[3], (SLICES, 3), 0, VARIANTS), jax.random.fold_in(key_list[3], 1), 0, VARIANTS - 1).astype(jnp.int32)
    mode_perms = jax.vmap(lambda own: jax.random.permutation(own, MODES))(jax.random.split(key_list[4], 3)).reshape((3, MODES)).astype(jnp.int32)
    owner_map = jax.random.permutation(key_list[5], N_CUTS).astype(jnp.int32)
    return dict(stems=stems, branches=branches, closing=closing, slice_values=slice_values, mode_perms=mode_perms, owner_map=owner_map)


def spread_order(perm, width):
    column = jnp.arange(width, dtype=jnp.int32)
    result = jnp.zeros((width,), jnp.int32)
    for bit in range(perm.shape[0]):
        moved = jnp.bitwise_and(jnp.right_shift(column, bit), 1)
        result = result + jnp.left_shift(moved, perm[bit].astype(jnp.int32))
    return result


def complex_block(pair):
    real_part = pair[0]
    imag_part = pair[1]
    top = jnp.concatenate([real_part, imag_part], axis=1)
    bottom = jnp.concatenate([-imag_part, real_part], axis=1)
    return jnp.concatenate([top, bottom], axis=0)


def relabel(amps):
    groups = N_STEM
    high = ROWS // groups
    narrow = WIDTH // groups
    parts = amps.reshape(groups, high, groups, 2, groups, narrow)
    parts = jnp.transpose(parts, (4, 0, 1, 3, 2, 5))
    return parts.reshape(groups, ROWS, 2, WIDTH)


def absorb(state, perm, pair):
    order = spread_order(perm, WIDTH)
    permuted = jnp.take(state, order, axis=3)
    flat = permuted.reshape(N_STEM * ROWS, 2 * WIDTH)
    out = jnp.dot(flat, complex_block(pair), preferred_element_type=jnp.float32)
    return out.astype(jnp.bfloat16)


def reference(stems, branches, closing, slice_values, mode_perms, owner_map):
    def one_slice(total, inputs):
        stem, values = inputs
        first = absorb(stem, mode_perms[0], branches[0, values[0]]).reshape(N_STEM, ROWS, 2, WIDTH)
        second = absorb(relabel(first), mode_perms[1], branches[1, values[1]]).reshape(N_STEM, ROWS, 2, WIDTH)
        final = absorb(relabel(second), mode_perms[2], closing[values[2]])
        final = final.reshape(N_STEM, ROWS, 2, HALF).astype(jnp.float32)
        return total + final, None

    start = jnp.zeros((N_STEM, ROWS, 2, HALF), jnp.float32)
    total, unused = lax.scan(one_slice, start, (stems, slice_values))
    blocks = total.reshape(N_STEM, ROWS, 2, N_CUTS, PIECE)
    blocks = jnp.take(blocks, owner_map.astype(jnp.int32), axis=3)
    return jnp.transpose(blocks, (0, 3, 2, 4, 1))
```

```python
import functools

import jax
import jax.numpy as jnp
from jax import lax
from jax.experimental import pallas as pl
from jax.experimental.pallas import tpu as pltpu
from jax.sharding import PartitionSpec as P


BF = jnp.bfloat16
F32 = jnp.float32
MESH = pl.DeviceIdType.MESH


def group_at(x, co, yy, zz):
    row = (yy + 2 + 4 * (x // 2)) % 8
    col = 2 * (co * 2 + x % 2) + 1 - zz
    return row * 8 + col


def place_of(group):
    row = group // 8
    col = group % 8
    turned = (row + 6) % 8
    zz = 1 - col % 2
    quarter = col // 2
    return (turned // 4) * 2 + quarter % 2, quarter // 2, turned % 4, zz


def spread(index, perms, which):
    total = jnp.zeros_like(index)
    for bit in range(9):
        moved = (index >> bit) & 1
        total = total + moved * (jnp.int32(1) << perms[which, bit])
    return total


def one_hot(rows, cols):
    return jnp.where(rows == cols, 1.0, 0.0).astype(BF)


def iota(shape, dim):
    return lax.broadcasted_iota(jnp.int32, shape, dim)


def mm(a, b):
    return jnp.dot(a, b, preferred_element_type=F32)


def turn(a, shift):
    return pltpu.roll(a, shift % 128, axis=a.ndim - 1)


def fold(direct, crossed, even):
    return direct + jnp.where(even, -turn(crossed, -1), turn(crossed, 1))


def kernel(chosen, perms, owners, x_hbm, br_hbm, cl_hbm, out_ref,
           xv, brv0, brv1, clv, sendbuf, recv1, fbuf, recv2, flag, flags, w3,
           lsem, send1, got1, send2, got2, sendf, gotf):
    cuts = lax.axis_index("cuts")
    stem = lax.axis_index("stem")
    zh, x, co = cuts // 8, (cuts // 2) % 4, cuts % 2
    y, zl = stem // 8, stem % 8
    yh, yy, zp, zz = y // 4, y % 4, zl // 2, zl % 2

    loads = [
        pltpu.make_async_copy(x_hbm, xv, lsem.at[0]),
        pltpu.make_async_copy(br_hbm.at[0], brv0, lsem.at[1]),
        pltpu.make_async_copy(br_hbm.at[1], brv1, lsem.at[2]),
        pltpu.make_async_copy(cl_hbm, clv, lsem.at[3]),
    ]
    for load in loads:
        load.start()

    def mate(step):
        dx, dc, dy, dz = step // 16, (step // 8) % 2, (step // 2) % 4, step % 2
        return (x + dx) % 4, (co + dc) % 2, (yy + dy) % 4, (zz + dz) % 2

    def device(px, pc, py, pz):
        return (zh * 8 + px * 2 + pc, yh * 32 + py * 8 + zp * 2 + pz)

    barrier = pltpu.get_barrier_semaphore()
    qx, qc, qy, qz = place_of(stem)

    def greet_source(pool, carry):
        pzh, pyh, pzp = pool // 8, (pool // 4) % 2, pool % 4
        pl.semaphore_signal(
            barrier, inc=1, device_id=(pzh * 8 + qx * 2 + qc, pyh * 32 + qy * 8 + pzp * 2 + qz), device_id_type=MESH
        )
        return carry

    lax.fori_loop(0, 16, greet_source, 0)

    def greet_mate(step, carry):
        pl.semaphore_signal(barrier, inc=1, device_id=device(*mate(step)), device_id_type=MESH)
        return carry

    lax.fori_loop(1, 64, greet_mate, 0)

    even = iota((1, 128), 1) % 2 == 0
    wide = iota((1, 512), 1)
    tall = iota((512, 512), 0)
    pick0 = one_hot(tall, spread(wide, perms, 0))
    part = iota((256, 256), 0)
    apart = one_hot((part % 128) * 2 + part // 128, iota((256, 256), 1))
    pair = (wide // 128) * 2 + wide % 2
    regroup = one_hot(tall, ((wide % 128) // 2) * 8 + pair)
    pick1 = one_hot((tall % 64) * 8 + tall // 64, spread(wide, perms, 1))

    flag[...] = jnp.full((8, 128), chosen[0, 2], jnp.int32).astype(F32)

    loads[0].wait()
    rows = xv[...].reshape(256, 512)
    rows = mm(apart, rows).astype(BF)
    rows = mm(rows, pick0).astype(BF)
    loads[1].wait()
    v0 = chosen[0, 0]
    y0 = mm(rows, brv0[v0, 0])
    y1 = mm(rows, brv0[v0, 1])
    a1 = jnp.concatenate([y0[:128] - y1[128:], y1[:128] + y0[128:]], axis=0).astype(BF)
    t = mm(a1, regroup)

    blocks = []
    for e2 in range(4):
        lanes = slice(e2 * 128, e2 * 128 + 128)
        low, high = [], []
        for h in range(2):
            re = t[h * 64:h * 64 + 64, lanes]
            im = t[128 + h * 64:192 + h * 64, lanes]
            low.append(jnp.where(even, re, turn(im, 1)))
            high.append(jnp.where(even, turn(re, -1), im))
        blocks.append(jnp.concatenate(low, axis=1))
        blocks.append(jnp.concatenate(high, axis=1))
    z = jnp.concatenate(blocks, axis=0).astype(BF)
    zq = lax.dot_general(pick1, z, (((0,), (0,)), ((), ())), preferred_element_type=F32).astype(BF)

    loads[2].wait()
    v1 = chosen[0, 1]
    t0 = lax.dot_general(brv1[v1, 0], zq, (((0,), (0,)), ((), ())), preferred_element_type=F32)
    t1 = lax.dot_general(brv1[v1, 1], zq, (((0,), (0,)), ((), ())), preferred_element_type=F32)
    halves = [
        fold(t0[:, h * 128:h * 128 + 128], t1[:, h * 128:h * 128 + 128], even).reshape(64, 8, 128) for h in range(2)
    ]
    sendbuf[...] = jnp.concatenate(halves, axis=1).astype(BF)

    pl.semaphore_wait(barrier, 79)

    mine = x * 2 + co

    def send_flag(step, carry):
        px, pc = (x + step // 2) % 4, (co + step % 2) % 2
        pltpu.make_async_remote_copy(
            src_ref=flag, dst_ref=flags.at[mine], send_sem=sendf, recv_sem=gotf,
            device_id=device(px, pc, yy, zz), device_id_type=MESH,
        ).start()
        return carry

    lax.fori_loop(1, 8, send_flag, 0)

    slot = mine * 8 + yy * 2 + zz

    def send_block(step, carry):
        px, pc, py, pz = mate(step)
        pltpu.make_async_remote_copy(
            src_ref=sendbuf.at[group_at(px, pc, py, pz)], dst_ref=recv1.at[slot], send_sem=send1, recv_sem=got1,
            device_id=device(px, pc, py, pz), device_id_type=MESH,
        ).start()
        return carry

    lax.fori_loop(1, 64, send_block, 0)
    recv1[slot] = sendbuf[group_at(x, co, yy, zz)]
    flags[mine] = flag[...]

    loads[3].wait()
    sub = iota((128, 512), 0)
    source = (((sub // 32) * 8 + zp * 2 + (sub // 16) % 2) * 2 + (sub // 8) % 2) * 8 + sub % 8
    pick2 = one_hot(source, spread(wide, perms, 2))
    column = iota((256, 256), 1)
    owner = jnp.zeros((1, 256), jnp.int32)
    block_of = iota((1, 256), 1) // 16
    for b in range(16):
        owner = jnp.where(block_of == b, owners[b], owner)
    deal = one_hot(iota((256, 256), 0), owner * 16 + iota((1, 256), 1) % 16)
    both = []
    for v in range(2):
        parts = [mm(mm(pick2, clv[v, q]).astype(BF), deal) for q in range(2)]
        both.append(jnp.concatenate(parts, axis=1).T)
    pltpu.make_async_copy(flags.at[pl.ds(0, 7)], flags.at[pl.ds(0, 7)], gotf).wait()
    for c in range(8):
        on = jnp.broadcast_to(flags[c][:1], (512, 128)) > 0.5
        w3[:, c * 128:c * 128 + 128] = jnp.where(on, both[1], both[0]).astype(BF)

    pltpu.make_async_copy(recv1.at[pl.ds(0, 63)], recv1.at[pl.ds(0, 63)], got1).wait()
    f = mm(w3[...], recv1[...].reshape(1024, 128))
    fbuf[...] = fold(f[:256], f[256:], even).reshape(16, 16, 128).astype(BF)

    group = group_at(x, co, yy, zz)
    pool = zh * 8 + yh * 4 + zp

    def send_part(step, carry):
        b = (cuts + 15 - step) % 16
        pltpu.make_async_remote_copy(
            src_ref=fbuf.at[b], dst_ref=recv2.at[pool], send_sem=send2, recv_sem=got2,
            device_id=(b, group), device_id_type=MESH,
        ).start()
        return carry

    lax.fori_loop(0, 16, send_part, 0)
    pltpu.make_async_copy(recv2, recv2, got2).wait()
    sums = []
    for h in range(2):
        total = jnp.zeros((16, 128), F32)
        for z2 in range(2):
            for k in range(4):
                total = total + recv2[z2 * 8 + h * 4 + k].astype(F32)
        sums.append(total)
    out_ref[0] = jnp.where(even, sums[0], turn(sums[1], 1))
    out_ref[1] = jnp.where(even, turn(sums[0], -1), sums[1])

    pltpu.make_async_copy(flags.at[pl.ds(0, 7)], flags.at[pl.ds(0, 7)], sendf).wait()
    pltpu.make_async_copy(sendbuf.at[pl.ds(0, 63)], sendbuf.at[pl.ds(0, 63)], send1).wait()
    pltpu.make_async_copy(fbuf, fbuf, send2).wait()


def body(stems, branches, closing, slice_values, mode_perms, owner_map):
    smem = pl.BlockSpec(memory_space=pltpu.SMEM)
    hbm = pl.BlockSpec(memory_space=pl.ANY)
    out = pl.pallas_call(
        kernel,
        out_shape=jax.ShapeDtypeStruct((2, 16, 128), F32),
        in_specs=[smem, smem, smem, hbm, hbm, hbm],
        out_specs=pl.BlockSpec(memory_space=pltpu.VMEM),
        scratch_shapes=[
            pltpu.VMEM((128, 2, 512), BF),
            pltpu.VMEM((2, 2, 512, 512), BF),
            pltpu.VMEM((2, 2, 512, 512), BF),
            pltpu.VMEM((2, 2, 512, 256), BF),
            pltpu.VMEM((64, 16, 128), BF),
            pltpu.VMEM((64, 16, 128), BF),
            pltpu.VMEM((16, 16, 128), BF),
            pltpu.VMEM((16, 16, 128), BF),
            pltpu.VMEM((8, 128), F32),
            pltpu.VMEM((8, 8, 128), F32),
            pltpu.VMEM((512, 1024), BF),
            pltpu.SemaphoreType.DMA((4,)),
            pltpu.SemaphoreType.DMA,
            pltpu.SemaphoreType.DMA,
            pltpu.SemaphoreType.DMA,
            pltpu.SemaphoreType.DMA,
            pltpu.SemaphoreType.DMA,
            pltpu.SemaphoreType.DMA,
        ],
        compiler_params=pltpu.CompilerParams(collective_id=0, has_side_effects=True),
    )(slice_values, mode_perms, owner_map, stems.reshape(128, 2, 512), branches, closing)
    return out.reshape(1, 1, 2, 16, 128)


def solution(mesh):
    in_specs = (P("cuts", "stem", None, None, None), P(), P(), P("cuts", None), P(), P())
    out_specs = P("stem", "cuts", None, None, None)
    return jax.shard_map(body, mesh=mesh, in_specs=in_specs, out_specs=out_specs, check_vma=False)
```

```python
import functools

import jax
import jax.numpy as jnp
from jax import lax
from jax.experimental import pallas as pl
from jax.experimental.pallas import tpu as pltpu
from jax.sharding import PartitionSpec as P


BF = jnp.bfloat16
F32 = jnp.float32
MESH = pl.DeviceIdType.MESH

FAR_FIRST = [(2, 2), (2, 1), (2, 3), (1, 2), (3, 2), (1, 1), (1, 3), (3, 1), (3, 3),
             (2, 0), (1, 0), (3, 0), (0, 2), (0, 1), (0, 3), (0, 0)]


def group_at(x, co, yy, zz):
    row = (yy + 2 + 4 * (x // 2)) % 8
    col = 2 * (co * 2 + x % 2) + 1 - zz
    return row * 8 + col


def place_of(group):
    row = group // 8
    col = group % 8
    turned = (row + 6) % 8
    zz = 1 - col % 2
    quarter = col // 2
    return (turned // 4) * 2 + quarter % 2, quarter // 2, turned % 4, zz


def spread(index, perms, which):
    total = jnp.zeros_like(index)
    for bit in range(9):
        moved = (index >> bit) & 1
        total = total + moved * (jnp.int32(1) << perms[which, bit])
    return total


def one_hot(rows, cols):
    return jnp.where(rows == cols, 1.0, 0.0).astype(BF)


def iota(shape, dim):
    return lax.broadcasted_iota(jnp.int32, shape, dim)


def mm(a, b):
    return jnp.dot(a, b, preferred_element_type=F32)


def turn(a, shift):
    return pltpu.roll(a, shift % 128, axis=a.ndim - 1)


def fold(direct, crossed, even):
    return direct + jnp.where(even, -turn(crossed, -1), turn(crossed, 1))


def kernel(chosen, perms, owners, x_hbm, br_hbm, cl_hbm, out_ref,
           xv, brv0, brv1, clv, sendbuf, recv1, fbuf, recv2, flag, flags, w3,
           lsem, send1, got1, send2, got2, sendf, gotf):
    cuts = lax.axis_index("cuts")
    stem = lax.axis_index("stem")
    zh, x, co = cuts // 8, (cuts // 2) % 4, cuts % 2
    y, zl = stem // 8, stem % 8
    yh, yy, zp, zz = y // 4, y % 4, zl // 2, zl % 2

    loads = [
        pltpu.make_async_copy(x_hbm, xv, lsem.at[0]),
        pltpu.make_async_copy(br_hbm.at[0], brv0, lsem.at[1]),
        pltpu.make_async_copy(br_hbm.at[1], brv1, lsem.at[2]),
        pltpu.make_async_copy(cl_hbm, clv, lsem.at[3]),
    ]
    for load in loads:
        load.start()

    xs = [lax.rem(x + d, 4) for d in range(4)]
    cs = [co, 1 - co]
    ys = [lax.rem(yy + d, 4) for d in range(4)]
    zs = [zz, 1 - zz]
    cut_of = [[zh * 8 + px * 2 + pc for pc in cs] for px in xs]
    stem_of = [[yh * 32 + py * 8 + zp * 2 + pz for pz in zs] for py in ys]
    mates = [(dx, dy, dc, dz) for dx, dy in FAR_FIRST for dc in (1, 0) for dz in (1, 0)][:-1]

    barrier = pltpu.get_barrier_semaphore()
    qx, qc, qy, qz = place_of(stem)
    for pzh in range(2):
        for pyh in range(2):
            for pzp in range(4):
                there = (pzh * 8 + qx * 2 + qc, pyh * 32 + qy * 8 + pzp * 2 + qz)
                pl.semaphore_signal(barrier, inc=1, device_id=there, device_id_type=MESH)
    for dx, dy, dc, dz in mates:
        there = (cut_of[dx][dc], stem_of[dy][dz])
        pl.semaphore_signal(barrier, inc=1, device_id=there, device_id_type=MESH)

    even = iota((1, 128), 1) % 2 == 0
    wide = iota((1, 512), 1)
    tall = iota((512, 512), 0)
    pick0 = one_hot(tall, spread(wide, perms, 0))
    part = iota((256, 256), 0)
    apart = one_hot((part % 128) * 2 + part // 128, iota((256, 256), 1))
    pair = (wide // 128) * 2 + wide % 2
    regroup = one_hot(tall, ((wide % 128) // 2) * 8 + pair)
    pick1 = one_hot((tall % 64) * 8 + tall // 64, spread(wide, perms, 1))

    flag[...] = jnp.full((8, 128), chosen[0, 2], jnp.int32).astype(F32)

    loads[0].wait()
    rows = xv[...].reshape(256, 512)
    rows = mm(apart, rows).astype(BF)
    rows = mm(rows, pick0).astype(BF)
    loads[1].wait()
    v0 = chosen[0, 0]
    y0 = mm(rows, brv0[v0, 0])
    y1 = mm(rows, brv0[v0, 1])
    a1 = jnp.concatenate([y0[:128] - y1[128:], y1[:128] + y0[128:]], axis=0).astype(BF)
    t = mm(a1, regroup)

    blocks = []
    for e2 in range(4):
        lanes = slice(e2 * 128, e2 * 128 + 128)
        low, high = [], []
        for h in range(2):
            re = t[h * 64:h * 64 + 64, lanes]
            im = t[128 + h * 64:192 + h * 64, lanes]
            low.append(jnp.where(even, re, turn(im, 1)))
            high.append(jnp.where(even, turn(re, -1), im))
        blocks.append(jnp.concatenate(low, axis=1))
        blocks.append(jnp.concatenate(high, axis=1))
    z = jnp.concatenate(blocks, axis=0).astype(BF)
    zq = lax.dot_general(pick1, z, (((0,), (0,)), ((), ())), preferred_element_type=F32).astype(BF)

    loads[2].wait()
    v1 = chosen[0, 1]
    t0 = lax.dot_general(brv1[v1, 0], zq, (((0,), (0,)), ((), ())), preferred_element_type=F32)
    t1 = lax.dot_general(brv1[v1, 1], zq, (((0,), (0,)), ((), ())), preferred_element_type=F32)
    halves = [
        fold(t0[:, h * 128:h * 128 + 128], t1[:, h * 128:h * 128 + 128], even).reshape(64, 8, 128) for h in range(2)
    ]
    sendbuf[...] = jnp.concatenate(halves, axis=1).astype(BF)

    pl.semaphore_wait(barrier, 79)

    mine = x * 2 + co

    slot = mine * 8 + yy * 2 + zz
    for dx, dc in ((2, 1), (2, 0), (1, 1), (1, 0), (3, 1), (3, 0), (0, 1)):
        pltpu.make_async_remote_copy(
            src_ref=flag, dst_ref=flags.at[mine], send_sem=sendf, recv_sem=gotf,
            device_id=(cut_of[dx][dc], stem_of[0][0]), device_id_type=MESH,
        ).start()
    halves_of = [px // 2 for px in xs]
    cols = [[4 * pc + 2 * (px - 2 * half) + 1 for pc in cs] for px, half in zip(xs, halves_of)]
    rows_of = [lax.rem(py + 2, 8) * 8 for py in ys]
    flips = [lax.rem(py + 6, 8) * 8 - row for py, row in zip(ys, rows_of)]
    for dx, dy, dc, dz in mates:
        theirs = rows_of[dy] + halves_of[dx] * flips[dy] + cols[dx][dc] - zs[dz]
        pltpu.make_async_remote_copy(
            src_ref=sendbuf.at[theirs], dst_ref=recv1.at[slot], send_sem=send1, recv_sem=got1.at[dx],
            device_id=(cut_of[dx][dc], stem_of[dy][dz]), device_id_type=MESH,
        ).start()
    recv1[slot] = sendbuf[group_at(x, co, yy, zz)]
    flags[mine] = flag[...]

    loads[3].wait()
    sub = iota((128, 512), 0)
    source = (((sub // 32) * 8 + zp * 2 + (sub // 16) % 2) * 2 + (sub // 8) % 2) * 8 + sub % 8
    pick2 = one_hot(source, spread(wide, perms, 2))
    column = iota((256, 256), 1)
    owner = jnp.zeros((1, 256), jnp.int32)
    block_of = iota((1, 256), 1) // 16
    for b in range(16):
        owner = jnp.where(block_of == b, owners[b], owner)
    deal = one_hot(iota((256, 256), 0), owner * 16 + iota((1, 256), 1) % 16)
    both = []
    for v in range(2):
        parts = [mm(mm(pick2, clv[v, q]).astype(BF), deal) for q in range(2)]
        both.append(jnp.concatenate(parts, axis=1).T)
    pltpu.make_async_copy(flags.at[pl.ds(0, 7)], flags.at[pl.ds(0, 7)], gotf).wait()
    for c in range(8):
        on = jnp.broadcast_to(flags[c][:1], (512, 128)) > 0.5
        w3[c // 2, :, (c % 2) * 128:(c % 2) * 128 + 128] = jnp.where(on, both[1], both[0]).astype(BF)

    f = None
    for dx in (2, 1, 3, 0):
        px = xs[(4 - dx) % 4]
        came = recv1.at[pl.ds(px * 16, 16 if dx else 15)]
        pltpu.make_async_copy(came, came, got1.at[dx]).wait()
        term = mm(w3[px], recv1[pl.ds(px * 16, 16)].reshape(256, 128))
        f = term if f is None else f + term
    fbuf[...] = fold(f[:256], f[256:], even).reshape(16, 16, 128).astype(BF)

    group = group_at(x, co, yy, zz)
    pool = zh * 8 + yh * 4 + zp

    for pzh in range(2):
        for dx in (2, 1, 3, 0):
            for dc in (1, 0):
                b = pzh * 8 + xs[dx] * 2 + cs[dc]
                pltpu.make_async_remote_copy(
                    src_ref=fbuf.at[b], dst_ref=recv2.at[pool], send_sem=send2, recv_sem=got2,
                    device_id=(b, group), device_id_type=MESH,
                ).start()
    pltpu.make_async_copy(recv2, recv2, got2).wait()
    sums = []
    for h in range(2):
        total = jnp.zeros((16, 128), F32)
        for z2 in range(2):
            for k in range(4):
                total = total + recv2[z2 * 8 + h * 4 + k].astype(F32)
        sums.append(total)
    out_ref[0] = jnp.where(even, sums[0], turn(sums[1], 1))
    out_ref[1] = jnp.where(even, turn(sums[0], -1), sums[1])

    pltpu.make_async_copy(flags.at[pl.ds(0, 7)], flags.at[pl.ds(0, 7)], sendf).wait()
    pltpu.make_async_copy(sendbuf.at[pl.ds(0, 63)], sendbuf.at[pl.ds(0, 63)], send1).wait()
    pltpu.make_async_copy(fbuf, fbuf, send2).wait()


def body(stems, branches, closing, slice_values, mode_perms, owner_map):
    smem = pl.BlockSpec(memory_space=pltpu.SMEM)
    hbm = pl.BlockSpec(memory_space=pl.ANY)
    out = pl.pallas_call(
        kernel,
        out_shape=jax.ShapeDtypeStruct((2, 16, 128), F32),
        in_specs=[smem, smem, smem, hbm, hbm, hbm],
        out_specs=pl.BlockSpec(memory_space=pltpu.VMEM),
        scratch_shapes=[
            pltpu.VMEM((128, 2, 512), BF),
            pltpu.VMEM((2, 2, 512, 512), BF),
            pltpu.VMEM((2, 2, 512, 512), BF),
            pltpu.VMEM((2, 2, 512, 256), BF),
            pltpu.VMEM((64, 16, 128), BF),
            pltpu.VMEM((64, 16, 128), BF),
            pltpu.VMEM((16, 16, 128), BF),
            pltpu.VMEM((16, 16, 128), BF),
            pltpu.VMEM((8, 128), F32),
            pltpu.VMEM((8, 8, 128), F32),
            pltpu.VMEM((4, 512, 256), BF),
            pltpu.SemaphoreType.DMA((4,)),
            pltpu.SemaphoreType.DMA,
            pltpu.SemaphoreType.DMA((4,)),
            pltpu.SemaphoreType.DMA,
            pltpu.SemaphoreType.DMA,
            pltpu.SemaphoreType.DMA,
            pltpu.SemaphoreType.DMA,
        ],
        compiler_params=pltpu.CompilerParams(collective_id=0, has_side_effects=True),
    )(slice_values, mode_perms, owner_map, stems.reshape(128, 2, 512), branches, closing)
    return out.reshape(1, 1, 2, 16, 128)


def solution(mesh):
    in_specs = (P("cuts", "stem", None, None, None), P(), P(), P("cuts", None), P(), P())
    out_specs = P("stem", "cuts", None, None, None)
    return jax.shard_map(body, mesh=mesh, in_specs=in_specs, out_specs=out_specs, check_vma=False)
```

```python
import functools

import jax
import jax.numpy as jnp
from jax import lax
from jax.experimental import pallas as pl
from jax.experimental.pallas import tpu as pltpu
from jax.sharding import PartitionSpec as P


BF = jnp.bfloat16
F32 = jnp.float32
MESH = pl.DeviceIdType.MESH

FAR_FIRST = [(2, 2), (2, 1), (2, 3), (1, 2), (3, 2), (1, 1), (1, 3), (3, 1), (3, 3),
             (2, 0), (1, 0), (3, 0), (0, 2), (0, 1), (0, 3), (0, 0)]


def group_at(x, co, yy, zz):
    row = (yy + 2 + 4 * (x // 2)) % 8
    col = 2 * (co * 2 + x % 2) + 1 - zz
    return row * 8 + col


def place_of(group):
    row = group // 8
    col = group % 8
    turned = (row + 6) % 8
    zz = 1 - col % 2
    quarter = col // 2
    return (turned // 4) * 2 + quarter % 2, quarter // 2, turned % 4, zz


def spread(index, perms, which):
    total = jnp.zeros_like(index)
    for bit in range(9):
        moved = (index >> bit) & 1
        total = total + moved * (jnp.int32(1) << perms[which, bit])
    return total


def one_hot(rows, cols):
    return jnp.where(rows == cols, 1.0, 0.0).astype(BF)


def iota(shape, dim):
    return lax.broadcasted_iota(jnp.int32, shape, dim)


def mm(a, b):
    return jnp.dot(a, b, preferred_element_type=F32)


def turn(a, shift):
    return pltpu.roll(a, shift % 128, axis=a.ndim - 1)


def fold(direct, crossed, even):
    return direct + jnp.where(even, -turn(crossed, -1), turn(crossed, 1))


def kernel(chosen_hbm, perms_hbm, owners_hbm, x_hbm, br_hbm, cl_hbm, out_ref,
           xv, brv0, brv1, clv, sendbuf, recv1, fbuf, recv2, flag, flags, w3, chosen, perms, owners,
           lsem, send1, got1, send2, got2, sendf, gotf, ready):
    cuts = lax.axis_index("cuts")
    stem = lax.axis_index("stem")
    zh, x, co = cuts // 8, (cuts // 2) % 4, cuts % 2
    y, zl = stem // 8, stem % 8
    yh, yy, zp, zz = y // 4, y % 4, zl // 2, zl % 2

    loads = [
        pltpu.make_async_copy(x_hbm, xv, lsem.at[0]),
        pltpu.make_async_copy(br_hbm.at[0], brv0, lsem.at[1]),
        pltpu.make_async_copy(br_hbm.at[1], brv1, lsem.at[2]),
        pltpu.make_async_copy(cl_hbm, clv, lsem.at[3]),
    ]
    tables = [
        pltpu.make_async_copy(chosen_hbm, chosen, lsem.at[4]),
        pltpu.make_async_copy(perms_hbm, perms, lsem.at[5]),
        pltpu.make_async_copy(owners_hbm, owners, lsem.at[6]),
    ]
    for load in tables + loads:
        load.start()

    xs = [lax.rem(x + d, 4) for d in range(4)]
    cs = [co, 1 - co]
    ys = [lax.rem(yy + d, 4) for d in range(4)]
    zs = [zz, 1 - zz]
    cut_of = [[zh * 8 + px * 2 + pc for pc in cs] for px in xs]
    stem_of = [[yh * 32 + py * 8 + zp * 2 + pz for pz in zs] for py in ys]
    mates = [(dx, dy, dc, dz) for dx, dy in FAR_FIRST for dc in (1, 0) for dz in (1, 0)][:-1]

    barrier = pltpu.get_barrier_semaphore()
    qx, qc, qy, qz = place_of(stem)
    height = zh * 8 + zl
    group = group_at(x, co, yy, zz)
    owner_z = [lax.rem(group, 8), lax.rem(group, 8) + 8]
    source_z = [(pzh, pzp, pzh * 8 + pzp * 2 + qz) for pzh in range(2) for pzp in range(4)]
    due = jnp.int32(63)
    for pzh, pzp, there_z in source_z:
        due = due + jnp.where(there_z < height, 2, 0)

        @pl.when(there_z > height)
        def _(pzh=pzh, pzp=pzp):
            for pyh in range(2):
                there = (pzh * 8 + qx * 2 + qc, pyh * 32 + qy * 8 + pzp * 2 + qz)
                pl.semaphore_signal(barrier, inc=1, device_id=there, device_id_type=MESH)

    for pzh in range(2):
        due = due + jnp.where(owner_z[pzh] < height, 8, 0)

        @pl.when(owner_z[pzh] > height)
        def _(pzh=pzh):
            for px in xs:
                for pc in cs:
                    there = (pzh * 8 + px * 2 + pc, group)
                    pl.semaphore_signal(barrier, inc=1, device_id=there, device_id_type=MESH)

    for dx, dy, dc, dz in mates:
        there = (cut_of[dx][dc], stem_of[dy][dz])
        pl.semaphore_signal(barrier, inc=1, device_id=there, device_id_type=MESH)

    for table in tables:
        table.wait()
    even = iota((1, 128), 1) % 2 == 0
    wide = iota((1, 512), 1)
    tall = iota((512, 512), 0)
    pick0 = one_hot(tall, spread(wide, perms, 0))
    part = iota((256, 256), 0)
    apart = one_hot((part % 128) * 2 + part // 128, iota((256, 256), 1))
    pair = (wide // 128) * 2 + wide % 2
    regroup = one_hot(tall, ((wide % 128) // 2) * 8 + pair)
    pick1 = one_hot((tall % 64) * 8 + tall // 64, spread(wide, perms, 1))

    flag[...] = jnp.full((8, 128), chosen[0, 2], jnp.int32).astype(F32)

    loads[0].wait()
    rows = xv[...].reshape(256, 512)
    rows = mm(apart, rows).astype(BF)
    rows = mm(rows, pick0).astype(BF)
    loads[1].wait()
    v0 = chosen[0, 0]
    y0 = mm(rows, brv0[v0, 0])
    y1 = mm(rows, brv0[v0, 1])
    a1 = jnp.concatenate([y0[:128] - y1[128:], y1[:128] + y0[128:]], axis=0).astype(BF)
    t = mm(a1, regroup)

    blocks = []
    for e2 in range(4):
        lanes = slice(e2 * 128, e2 * 128 + 128)
        low, high = [], []
        for h in range(2):
            re = t[h * 64:h * 64 + 64, lanes]
            im = t[128 + h * 64:192 + h * 64, lanes]
            low.append(jnp.where(even, re, turn(im, 1)))
            high.append(jnp.where(even, turn(re, -1), im))
        blocks.append(jnp.concatenate(low, axis=1))
        blocks.append(jnp.concatenate(high, axis=1))
    z = jnp.concatenate(blocks, axis=0).astype(BF)
    zq = lax.dot_general(pick1, z, (((0,), (0,)), ((), ())), preferred_element_type=F32).astype(BF)

    loads[2].wait()
    v1 = chosen[0, 1]
    t0 = lax.dot_general(brv1[v1, 0], zq, (((0,), (0,)), ((), ())), preferred_element_type=F32)
    t1 = lax.dot_general(brv1[v1, 1], zq, (((0,), (0,)), ((), ())), preferred_element_type=F32)
    halves = [
        fold(t0[:, h * 128:h * 128 + 128], t1[:, h * 128:h * 128 + 128], even).reshape(64, 8, 128) for h in range(2)
    ]
    sendbuf[...] = jnp.concatenate(halves, axis=1).astype(BF)

    pl.semaphore_wait(barrier, due)

    mine = x * 2 + co

    slot = mine * 8 + yy * 2 + zz
    for dx, dc in ((2, 1), (2, 0), (1, 1), (1, 0), (3, 1), (3, 0), (0, 1)):
        pltpu.make_async_remote_copy(
            src_ref=flag, dst_ref=flags.at[mine], send_sem=sendf, recv_sem=gotf,
            device_id=(cut_of[dx][dc], stem_of[0][0]), device_id_type=MESH,
        ).start()
    halves_of = [px // 2 for px in xs]
    cols = [[4 * pc + 2 * (px - 2 * half) + 1 for pc in cs] for px, half in zip(xs, halves_of)]
    rows_of = [lax.rem(py + 2, 8) * 8 for py in ys]
    flips = [lax.rem(py + 6, 8) * 8 - row for py, row in zip(ys, rows_of)]
    for dx, dy, dc, dz in mates:
        theirs = rows_of[dy] + halves_of[dx] * flips[dy] + cols[dx][dc] - zs[dz]
        pltpu.make_async_remote_copy(
            src_ref=sendbuf.at[theirs], dst_ref=recv1.at[slot], send_sem=send1, recv_sem=got1.at[dx],
            device_id=(cut_of[dx][dc], stem_of[dy][dz]), device_id_type=MESH,
        ).start()
    for pzh, pzp, there_z in source_z:

        @pl.when(there_z < height)
        def _(pzh=pzh, pzp=pzp):
            for pyh in range(2):
                there = (pzh * 8 + qx * 2 + qc, pyh * 32 + qy * 8 + pzp * 2 + qz)
                pl.semaphore_signal(ready.at[zh], inc=1, device_id=there, device_id_type=MESH)

    recv1[slot] = sendbuf[group]
    flags[mine] = flag[...]

    loads[3].wait()
    sub = iota((128, 512), 0)
    source = (((sub // 32) * 8 + zp * 2 + (sub // 16) % 2) * 2 + (sub // 8) % 2) * 8 + sub % 8
    pick2 = one_hot(source, spread(wide, perms, 2))
    column = iota((256, 256), 1)
    owner = jnp.zeros((1, 256), jnp.int32)
    block_of = iota((1, 256), 1) // 16
    for b in range(16):
        owner = jnp.where(block_of == b, owners[b], owner)
    deal = one_hot(iota((256, 256), 0), owner * 16 + iota((1, 256), 1) % 16)
    both = []
    for v in range(2):
        parts = [mm(mm(pick2, clv[v, q]).astype(BF), deal) for q in range(2)]
        both.append(jnp.concatenate(parts, axis=1).T)
    pltpu.make_async_copy(flags.at[pl.ds(0, 7)], flags.at[pl.ds(0, 7)], gotf).wait()
    for c in range(8):
        on = jnp.broadcast_to(flags[c][:1], (512, 128)) > 0.5
        w3[c // 2, :, (c % 2) * 128:(c % 2) * 128 + 128] = jnp.where(on, both[1], both[0]).astype(BF)

    f = None
    for dx in (2, 1, 3, 0):
        px = xs[(4 - dx) % 4]
        came = recv1.at[pl.ds(px * 16, 16 if dx else 15)]
        pltpu.make_async_copy(came, came, got1.at[dx]).wait()
        term = mm(w3[px], recv1[pl.ds(px * 16, 16)].reshape(256, 128))
        f = term if f is None else f + term
    fbuf[...] = fold(f[:256], f[256:], even).reshape(16, 16, 128).astype(BF)

    pool = zh * 8 + yh * 4 + zp

    for pzh in range(2):

        @pl.when(owner_z[pzh] > height)
        def _(pzh=pzh):
            pl.semaphore_wait(ready.at[pzh], 8)

        for dx in (2, 1, 3, 0):
            for dc in (1, 0):
                b = pzh * 8 + xs[dx] * 2 + cs[dc]
                pltpu.make_async_remote_copy(
                    src_ref=fbuf.at[b], dst_ref=recv2.at[pool], send_sem=send2, recv_sem=got2,
                    device_id=(b, group), device_id_type=MESH,
                ).start()
    pltpu.make_async_copy(recv2, recv2, got2).wait()
    sums = []
    for h in range(2):
        total = jnp.zeros((16, 128), F32)
        for z2 in range(2):
            for k in range(4):
                total = total + recv2[z2 * 8 + h * 4 + k].astype(F32)
        sums.append(total)
    out_ref[0] = jnp.where(even, sums[0], turn(sums[1], 1))
    out_ref[1] = jnp.where(even, turn(sums[0], -1), sums[1])

    pltpu.make_async_copy(flags.at[pl.ds(0, 7)], flags.at[pl.ds(0, 7)], sendf).wait()
    pltpu.make_async_copy(sendbuf.at[pl.ds(0, 63)], sendbuf.at[pl.ds(0, 63)], send1).wait()
    pltpu.make_async_copy(fbuf, fbuf, send2).wait()


def body(stems, branches, closing, slice_values, mode_perms, owner_map):
    hbm = pl.BlockSpec(memory_space=pl.ANY)
    out = pl.pallas_call(
        kernel,
        out_shape=jax.ShapeDtypeStruct((2, 16, 128), F32),
        in_specs=[hbm] * 6,
        out_specs=pl.BlockSpec(memory_space=pltpu.VMEM),
        scratch_shapes=[
            pltpu.VMEM((128, 2, 512), BF),
            pltpu.VMEM((2, 2, 512, 512), BF),
            pltpu.VMEM((2, 2, 512, 512), BF),
            pltpu.VMEM((2, 2, 512, 256), BF),
            pltpu.VMEM((64, 16, 128), BF),
            pltpu.VMEM((64, 16, 128), BF),
            pltpu.VMEM((16, 16, 128), BF),
            pltpu.VMEM((16, 16, 128), BF),
            pltpu.VMEM((8, 128), F32),
            pltpu.VMEM((8, 8, 128), F32),
            pltpu.VMEM((4, 512, 256), BF),
            pltpu.SMEM((1, 3), jnp.int32),
            pltpu.SMEM((3, 9), jnp.int32),
            pltpu.SMEM((16,), jnp.int32),
            pltpu.SemaphoreType.DMA((7,)),
            pltpu.SemaphoreType.DMA,
            pltpu.SemaphoreType.DMA((4,)),
            pltpu.SemaphoreType.DMA,
            pltpu.SemaphoreType.DMA,
            pltpu.SemaphoreType.DMA,
            pltpu.SemaphoreType.DMA,
            pltpu.SemaphoreType.REGULAR((2,)),
        ],
        compiler_params=pltpu.CompilerParams(collective_id=0, has_side_effects=True),
    )(slice_values, mode_perms, owner_map, stems.reshape(128, 2, 512), branches, closing)
    return out.reshape(1, 1, 2, 16, 128)


def solution(mesh):
    in_specs = (P("cuts", "stem", None, None, None), P(), P(), P("cuts", None), P(), P())
    out_specs = P("stem", "cuts", None, None, None)
    return jax.shard_map(body, mesh=mesh, in_specs=in_specs, out_specs=out_specs, check_vma=False)
```

```python
import functools

import jax
import jax.numpy as jnp
from jax import lax
from jax.experimental import pallas as pl
from jax.experimental.pallas import tpu as pltpu
from jax.sharding import PartitionSpec as P


BF = jnp.bfloat16
F32 = jnp.float32
MESH = pl.DeviceIdType.MESH


def group_at(x, co, yy, zz):
    row = (yy + 2 + 4 * (x // 2)) % 8
    col = 2 * (co * 2 + x % 2) + 1 - zz
    return row * 8 + col


def place_of(group):
    row = group // 8
    col = group % 8
    turned = (row + 6) % 8
    zz = 1 - col % 2
    quarter = col // 2
    return (turned // 4) * 2 + quarter % 2, quarter // 2, turned % 4, zz


def spread(index, perms, which):
    total = jnp.zeros_like(index)
    for bit in range(9):
        moved = (index >> bit) & 1
        total = total + moved * (jnp.int32(1) << perms[which, bit])
    return total


def one_hot(rows, cols):
    return jnp.where(rows == cols, 1.0, 0.0).astype(BF)


def iota(shape, dim):
    return lax.broadcasted_iota(jnp.int32, shape, dim)


def mm(a, b):
    return jnp.dot(a, b, preferred_element_type=F32)


def turn(a, shift):
    return pltpu.roll(a, shift % 128, axis=a.ndim - 1)


def fold(direct, crossed, even):
    return direct + jnp.where(even, -turn(crossed, -1), turn(crossed, 1))


def kernel(chosen_hbm, perms_hbm, owners_hbm, x_hbm, br_hbm, cl_hbm, out_ref,
           xv, brv0, brv1, clv, sendbuf, recv1, fbuf, recv2, flag, flags, w3, chosen, perms, owners,
           lsem, send1, got1, send2, got2, sendf, gotf, ready, open1):
    cuts = lax.axis_index("cuts")
    stem = lax.axis_index("stem")
    zh, x, co = cuts // 8, (cuts // 2) % 4, cuts % 2
    y, zl = stem // 8, stem % 8
    yh, yy, zp, zz = y // 4, y % 4, zl // 2, zl % 2

    loads = [
        pltpu.make_async_copy(x_hbm, xv, lsem.at[0]),
        pltpu.make_async_copy(br_hbm.at[0], brv0, lsem.at[1]),
        pltpu.make_async_copy(br_hbm.at[1], brv1, lsem.at[2]),
        pltpu.make_async_copy(cl_hbm, clv, lsem.at[3]),
    ]
    tables = [
        pltpu.make_async_copy(chosen_hbm, chosen, lsem.at[4]),
        pltpu.make_async_copy(perms_hbm, perms, lsem.at[5]),
        pltpu.make_async_copy(owners_hbm, owners, lsem.at[6]),
    ]
    for load in tables + loads:
        load.start()

    xs = [lax.rem(x + d, 4) for d in range(4)]
    cs = [co, 1 - co]
    ys = [lax.rem(yy + d, 4) for d in range(4)]
    zs = [zz, 1 - zz]
    cut_of = [[zh * 8 + px * 2 + pc for pc in cs] for px in xs]
    stem_of = [[yh * 32 + py * 8 + zp * 2 + pz for pz in zs] for py in ys]
    crowd = [(dx, dc, dz) for dx in (2, 1, 3, 0) for dc in (1, 0) for dz in (1, 0)]
    rank_of = [jnp.where(yh == 0, py, 3 - py) for py in ys]

    barrier = pltpu.get_barrier_semaphore()
    qx, qc, qy, qz = place_of(stem)
    height = zh * 8 + zl
    group = group_at(x, co, yy, zz)
    owner_z = [lax.rem(group, 8), lax.rem(group, 8) + 8]
    source_z = [(pzh, pzp, pzh * 8 + pzp * 2 + qz) for pzh in range(2) for pzp in range(4)]
    due = jnp.int32(15)
    for pzh, pzp, there_z in source_z:
        due = due + jnp.where(there_z < height, 2, 0)

        @pl.when(there_z > height)
        def _(pzh=pzh, pzp=pzp):
            for pyh in range(2):
                there = (pzh * 8 + qx * 2 + qc, pyh * 32 + qy * 8 + pzp * 2 + qz)
                pl.semaphore_signal(barrier, inc=1, device_id=there, device_id_type=MESH)

    for pzh in range(2):
        due = due + jnp.where(owner_z[pzh] < height, 8, 0)

        @pl.when(owner_z[pzh] > height)
        def _(pzh=pzh):
            for px in xs:
                for pc in cs:
                    there = (pzh * 8 + px * 2 + pc, group)
                    pl.semaphore_signal(barrier, inc=1, device_id=there, device_id_type=MESH)

    for dx, dc, dz in crowd[:-1]:
        pl.semaphore_signal(barrier, inc=1, device_id=(cut_of[dx][dc], stem_of[0][dz]), device_id_type=MESH)
    for dy in (1, 2, 3):
        due = due + jnp.where(rank_of[dy] < rank_of[0], 16, 0)

        @pl.when(rank_of[dy] > rank_of[0])
        def _(dy=dy):
            for dx, dc, dz in crowd:
                pl.semaphore_signal(barrier, inc=1, device_id=(cut_of[dx][dc], stem_of[dy][dz]), device_id_type=MESH)

    for table in tables:
        table.wait()
    even = iota((1, 128), 1) % 2 == 0
    wide = iota((1, 512), 1)
    tall = iota((512, 512), 0)
    pick0 = one_hot(tall, spread(wide, perms, 0))
    part = iota((256, 256), 0)
    apart = one_hot((part % 128) * 2 + part // 128, iota((256, 256), 1))
    pair = (wide // 128) * 2 + wide % 2
    regroup = one_hot(tall, ((wide % 128) // 2) * 8 + pair)
    pick1 = one_hot((tall % 64) * 8 + tall // 64, spread(wide, perms, 1))

    flag[...] = jnp.full((8, 128), chosen[0, 2], jnp.int32).astype(F32)

    loads[0].wait()
    rows = xv[...].reshape(256, 512)
    rows = mm(apart, rows).astype(BF)
    rows = mm(rows, pick0).astype(BF)
    loads[1].wait()
    v0 = chosen[0, 0]
    y0 = mm(rows, brv0[v0, 0])
    y1 = mm(rows, brv0[v0, 1])
    a1 = jnp.concatenate([y0[:128] - y1[128:], y1[:128] + y0[128:]], axis=0).astype(BF)
    t = mm(a1, regroup)

    blocks = []
    for e2 in range(4):
        lanes = slice(e2 * 128, e2 * 128 + 128)
        low, high = [], []
        for h in range(2):
            re = t[h * 64:h * 64 + 64, lanes]
            im = t[128 + h * 64:192 + h * 64, lanes]
            low.append(jnp.where(even, re, turn(im, 1)))
            high.append(jnp.where(even, turn(re, -1), im))
        blocks.append(jnp.concatenate(low, axis=1))
        blocks.append(jnp.concatenate(high, axis=1))
    z = jnp.concatenate(blocks, axis=0).astype(BF)
    zq = lax.dot_general(pick1, z, (((0,), (0,)), ((), ())), preferred_element_type=F32).astype(BF)

    pl.semaphore_wait(barrier, due)
    for dy in (1, 2, 3):

        @pl.when(rank_of[dy] < rank_of[0])
        def _(dy=dy):
            for dx, dc, dz in crowd:
                there = (cut_of[dx][dc], stem_of[dy][dz])
                pl.semaphore_signal(open1.at[4 - dy], inc=1, device_id=there, device_id_type=MESH)

    mine = x * 2 + co

    for dx, dc in ((2, 1), (2, 0), (1, 1), (1, 0), (3, 1), (3, 0), (0, 1)):
        pltpu.make_async_remote_copy(
            src_ref=flag, dst_ref=flags.at[mine], send_sem=sendf, recv_sem=gotf,
            device_id=(cut_of[dx][dc], stem_of[0][0]), device_id_type=MESH,
        ).start()

    for pzh, pzp, there_z in source_z:

        @pl.when(there_z < height)
        def _(pzh=pzh, pzp=pzp):
            for pyh in range(2):
                there = (pzh * 8 + qx * 2 + qc, pyh * 32 + qy * 8 + pzp * 2 + qz)
                pl.semaphore_signal(ready.at[zh], inc=1, device_id=there, device_id_type=MESH)

    loads[2].wait()
    v1 = chosen[0, 1]
    t0 = lax.dot_general(brv1[v1, 0], zq, (((0,), (0,)), ((), ())), preferred_element_type=F32)
    t1 = lax.dot_general(brv1[v1, 1], zq, (((0,), (0,)), ((), ())), preferred_element_type=F32)
    halves = [
        fold(t0[:, h * 128:h * 128 + 128], t1[:, h * 128:h * 128 + 128], even).reshape(64, 8, 128) for h in range(2)
    ]
    sendbuf[...] = jnp.concatenate(halves, axis=1).astype(BF)

    slot = mine * 8 + yy * 2 + zz
    halves_of = [px // 2 for px in xs]
    cols = [[4 * pc + 2 * (px - 2 * half) + 1 for pc in cs] for px, half in zip(xs, halves_of)]
    rows_of = [lax.rem(py + 2, 8) * 8 for py in ys]
    flips = [lax.rem(py + 6, 8) * 8 - row for py, row in zip(ys, rows_of)]

    def send_blocks(dy, group_of_mates):
        for dx, dc, dz in group_of_mates:
            theirs = rows_of[dy] + halves_of[dx] * flips[dy] + cols[dx][dc] - zs[dz]
            pltpu.make_async_remote_copy(
                src_ref=sendbuf.at[theirs], dst_ref=recv1.at[slot], send_sem=send1, recv_sem=got1.at[dx],
                device_id=(cut_of[dx][dc], stem_of[dy][dz]), device_id_type=MESH,
            ).start()

    for dy in (2, 1, 3):

        @pl.when(rank_of[dy] < rank_of[0])
        def _(dy=dy):
            send_blocks(dy, crowd)

    send_blocks(0, crowd[:-1])
    for dy in (2, 1, 3):

        @pl.when(rank_of[dy] > rank_of[0])
        def _(dy=dy):
            pl.semaphore_wait(open1.at[dy], 16)
            send_blocks(dy, crowd)

    recv1[slot] = sendbuf[group]
    flags[mine] = flag[...]

    loads[3].wait()
    sub = iota((128, 512), 0)
    source = (((sub // 32) * 8 + zp * 2 + (sub // 16) % 2) * 2 + (sub // 8) % 2) * 8 + sub % 8
    pick2 = one_hot(source, spread(wide, perms, 2))
    column = iota((256, 256), 1)
    owner = jnp.zeros((1, 256), jnp.int32)
    block_of = iota((1, 256), 1) // 16
    for b in range(16):
        owner = jnp.where(block_of == b, owners[b], owner)
    deal = one_hot(iota((256, 256), 0), owner * 16 + iota((1, 256), 1) % 16)
    both = []
    for v in range(2):
        parts = [mm(mm(pick2, clv[v, q]).astype(BF), deal) for q in range(2)]
        both.append(jnp.concatenate(parts, axis=1).T)
    pltpu.make_async_copy(flags.at[pl.ds(0, 7)], flags.at[pl.ds(0, 7)], gotf).wait()
    for c in range(8):
        on = jnp.broadcast_to(flags[c][:1], (512, 128)) > 0.5
        w3[c // 2, :, (c % 2) * 128:(c % 2) * 128 + 128] = jnp.where(on, both[1], both[0]).astype(BF)

    f = None
    for dx in (2, 1, 3, 0):
        px = xs[(4 - dx) % 4]
        came = recv1.at[pl.ds(px * 16, 16 if dx else 15)]
        pltpu.make_async_copy(came, came, got1.at[dx]).wait()
        term = mm(w3[px], recv1[pl.ds(px * 16, 16)].reshape(256, 128))
        f = term if f is None else f + term
    fbuf[...] = fold(f[:256], f[256:], even).reshape(16, 16, 128).astype(BF)

    pool = zh * 8 + yh * 4 + zp

    for pzh in range(2):

        @pl.when(owner_z[pzh] > height)
        def _(pzh=pzh):
            pl.semaphore_wait(ready.at[pzh], 8)

        for dx in (2, 1, 3, 0):
            for dc in (1, 0):
                b = pzh * 8 + xs[dx] * 2 + cs[dc]
                pltpu.make_async_remote_copy(
                    src_ref=fbuf.at[b], dst_ref=recv2.at[pool], send_sem=send2, recv_sem=got2,
                    device_id=(b, group), device_id_type=MESH,
                ).start()
    pltpu.make_async_copy(recv2, recv2, got2).wait()
    sums = []
    for h in range(2):
        total = jnp.zeros((16, 128), F32)
        for z2 in range(2):
            for k in range(4):
                total = total + recv2[z2 * 8 + h * 4 + k].astype(F32)
        sums.append(total)
    out_ref[0] = jnp.where(even, sums[0], turn(sums[1], 1))
    out_ref[1] = jnp.where(even, turn(sums[0], -1), sums[1])

    pltpu.make_async_copy(flags.at[pl.ds(0, 7)], flags.at[pl.ds(0, 7)], sendf).wait()
    pltpu.make_async_copy(sendbuf.at[pl.ds(0, 63)], sendbuf.at[pl.ds(0, 63)], send1).wait()
    pltpu.make_async_copy(fbuf, fbuf, send2).wait()


def body(stems, branches, closing, slice_values, mode_perms, owner_map):
    hbm = pl.BlockSpec(memory_space=pl.ANY)
    out = pl.pallas_call(
        kernel,
        out_shape=jax.ShapeDtypeStruct((2, 16, 128), F32),
        in_specs=[hbm] * 6,
        out_specs=pl.BlockSpec(memory_space=pltpu.VMEM),
        scratch_shapes=[
            pltpu.VMEM((128, 2, 512), BF),
            pltpu.VMEM((2, 2, 512, 512), BF),
            pltpu.VMEM((2, 2, 512, 512), BF),
            pltpu.VMEM((2, 2, 512, 256), BF),
            pltpu.VMEM((64, 16, 128), BF),
            pltpu.VMEM((64, 16, 128), BF),
            pltpu.VMEM((16, 16, 128), BF),
            pltpu.VMEM((16, 16, 128), BF),
            pltpu.VMEM((8, 128), F32),
            pltpu.VMEM((8, 8, 128), F32),
            pltpu.VMEM((4, 512, 256), BF),
            pltpu.SMEM((1, 3), jnp.int32),
            pltpu.SMEM((3, 9), jnp.int32),
            pltpu.SMEM((16,), jnp.int32),
            pltpu.SemaphoreType.DMA((7,)),
            pltpu.SemaphoreType.DMA,
            pltpu.SemaphoreType.DMA((4,)),
            pltpu.SemaphoreType.DMA,
            pltpu.SemaphoreType.DMA,
            pltpu.SemaphoreType.DMA,
            pltpu.SemaphoreType.DMA,
            pltpu.SemaphoreType.REGULAR((2,)),
            pltpu.SemaphoreType.REGULAR((4,)),
        ],
        compiler_params=pltpu.CompilerParams(collective_id=0, has_side_effects=True),
    )(slice_values, mode_perms, owner_map, stems.reshape(128, 2, 512), branches, closing)
    return out.reshape(1, 1, 2, 16, 128)


def solution(mesh):
    in_specs = (P("cuts", "stem", None, None, None), P(), P(), P("cuts", None), P(), P())
    out_specs = P("stem", "cuts", None, None, None)
    return jax.shard_map(body, mesh=mesh, in_specs=in_specs, out_specs=out_specs, check_vma=False)
```

```python
import functools

import jax
import jax.numpy as jnp
from jax import lax
from jax.experimental import pallas as pl
from jax.experimental.pallas import tpu as pltpu
from jax.sharding import PartitionSpec as P


BF = jnp.bfloat16
F32 = jnp.float32
MESH = pl.DeviceIdType.MESH

FAR_FIRST = [(2, 2), (2, 1), (2, 3), (1, 2), (3, 2), (1, 1), (1, 3), (3, 1), (3, 3),
             (2, 0), (1, 0), (3, 0), (0, 2), (0, 1), (0, 3), (0, 0)]


def group_at(x, co, yy, zz):
    row = (yy + 2 + 4 * (x // 2)) % 8
    col = 2 * (co * 2 + x % 2) + 1 - zz
    return row * 8 + col


def place_of(group):
    row = group // 8
    col = group % 8
    turned = (row + 6) % 8
    zz = 1 - col % 2
    quarter = col // 2
    return (turned // 4) * 2 + quarter % 2, quarter // 2, turned % 4, zz


def spread(index, perms, which):
    total = jnp.zeros_like(index)
    for bit in range(9):
        moved = (index >> bit) & 1
        total = total + moved * (jnp.int32(1) << perms[which, bit])
    return total


def one_hot(rows, cols):
    return jnp.where(rows == cols, 1.0, 0.0).astype(BF)


def iota(shape, dim):
    return lax.broadcasted_iota(jnp.int32, shape, dim)


def mm(a, b):
    return jnp.dot(a, b, preferred_element_type=F32)


def turn(a, shift):
    return pltpu.roll(a, shift % 128, axis=a.ndim - 1)


def fold(direct, crossed, even):
    return direct + jnp.where(even, -turn(crossed, -1), turn(crossed, 1))


def kernel(chosen_hbm, perms_hbm, owners_hbm, x_hbm, br_hbm, cl_hbm, out_ref,
           xv, brv0, brv1, clv, sendbuf, recv1, fbuf, recv2, flag, flags, w3, chosen, perms, owners,
           lsem, send1, got1, send2, got2, sendf, gotf, ready):
    cuts = lax.axis_index("cuts")
    stem = lax.axis_index("stem")
    zh, x, co = cuts // 8, (cuts // 2) % 4, cuts % 2
    y, zl = stem // 8, stem % 8
    yh, yy, zp, zz = y // 4, y % 4, zl // 2, zl % 2

    loads = [
        pltpu.make_async_copy(x_hbm, xv, lsem.at[0]),
        pltpu.make_async_copy(br_hbm.at[0], brv0, lsem.at[1]),
        pltpu.make_async_copy(br_hbm.at[1], brv1, lsem.at[2]),
        pltpu.make_async_copy(cl_hbm, clv, lsem.at[3]),
    ]
    tables = [
        pltpu.make_async_copy(chosen_hbm, chosen, lsem.at[4]),
        pltpu.make_async_copy(perms_hbm, perms, lsem.at[5]),
        pltpu.make_async_copy(owners_hbm, owners, lsem.at[6]),
    ]
    for load in tables + loads:
        load.start()

    xs = [lax.rem(x + d, 4) for d in range(4)]
    cs = [co, 1 - co]
    ys = [lax.rem(yy + d, 4) for d in range(4)]
    zs = [zz, 1 - zz]
    cut_of = [[zh * 8 + px * 2 + pc for pc in cs] for px in xs]
    stem_of = [[yh * 32 + py * 8 + zp * 2 + pz for pz in zs] for py in ys]
    mates = [(dx, dy, dc, dz) for dx, dy in FAR_FIRST for dc in (1, 0) for dz in (1, 0)][:-1]

    barrier = pltpu.get_barrier_semaphore()
    qx, qc, qy, qz = place_of(stem)
    height = zh * 8 + zl
    group = group_at(x, co, yy, zz)
    owner_z = [lax.rem(group, 8), lax.rem(group, 8) + 8]
    source_z = [(pzh, pzp, pzh * 8 + pzp * 2 + qz) for pzh in range(2) for pzp in range(4)]
    due = jnp.int32(63)
    for pzh, pzp, there_z in source_z:
        due = due + jnp.where(there_z < height, 2, 0)

        @pl.when(there_z > height)
        def _(pzh=pzh, pzp=pzp):
            for pyh in range(2):
                there = (pzh * 8 + qx * 2 + qc, pyh * 32 + qy * 8 + pzp * 2 + qz)
                pl.semaphore_signal(barrier, inc=1, device_id=there, device_id_type=MESH)

    for pzh in range(2):
        due = due + jnp.where(owner_z[pzh] < height, 8, 0)

        @pl.when(owner_z[pzh] > height)
        def _(pzh=pzh):
            for px in xs:
                for pc in cs:
                    there = (pzh * 8 + px * 2 + pc, group)
                    pl.semaphore_signal(barrier, inc=1, device_id=there, device_id_type=MESH)

    for dx, dy, dc, dz in mates:
        there = (cut_of[dx][dc], stem_of[dy][dz])
        pl.semaphore_signal(barrier, inc=1, device_id=there, device_id_type=MESH)

    for table in tables:
        table.wait()
    even = iota((1, 128), 1) % 2 == 0
    wide = iota((1, 512), 1)
    tall = iota((512, 512), 0)
    pick0 = one_hot(tall, spread(wide, perms, 0))
    part = iota((256, 256), 0)
    apart = one_hot((part % 128) * 2 + part // 128, iota((256, 256), 1))
    pair = (wide // 128) * 2 + wide % 2
    regroup = one_hot(tall, ((wide % 128) // 2) * 8 + pair)
    pick1 = one_hot((tall % 64) * 8 + tall // 64, spread(wide, perms, 1))

    flag[...] = jnp.full((8, 128), chosen[0, 2], jnp.int32).astype(F32)

    loads[0].wait()
    rows = xv[...].reshape(256, 512)
    rows = mm(apart, rows).astype(BF)
    rows = mm(rows, pick0).astype(BF)
    loads[1].wait()
    v0 = chosen[0, 0]
    y0 = mm(rows, brv0[v0, 0])
    y1 = mm(rows, brv0[v0, 1])
    a1 = jnp.concatenate([y0[:128] - y1[128:], y1[:128] + y0[128:]], axis=0).astype(BF)
    t = mm(a1, regroup)

    blocks = []
    for e2 in range(4):
        lanes = slice(e2 * 128, e2 * 128 + 128)
        low, high = [], []
        for h in range(2):
            re = t[h * 64:h * 64 + 64, lanes]
            im = t[128 + h * 64:192 + h * 64, lanes]
            low.append(jnp.where(even, re, turn(im, 1)))
            high.append(jnp.where(even, turn(re, -1), im))
        blocks.append(jnp.concatenate(low, axis=1))
        blocks.append(jnp.concatenate(high, axis=1))
    z = jnp.concatenate(blocks, axis=0).astype(BF)
    zq = lax.dot_general(pick1, z, (((0,), (0,)), ((), ())), preferred_element_type=F32).astype(BF)

    loads[2].wait()
    v1 = chosen[0, 1]
    t0 = lax.dot_general(brv1[v1, 0], zq, (((0,), (0,)), ((), ())), preferred_element_type=F32)
    t1 = lax.dot_general(brv1[v1, 1], zq, (((0,), (0,)), ((), ())), preferred_element_type=F32)
    halves = [
        fold(t0[:, h * 128:h * 128 + 128], t1[:, h * 128:h * 128 + 128], even).reshape(64, 8, 128) for h in range(2)
    ]
    sendbuf[...] = jnp.concatenate(halves, axis=1).astype(BF)

    pl.semaphore_wait(barrier, due)

    mine = x * 2 + co

    slot = mine * 8 + yy * 2 + zz
    for dx, dc in ((2, 1), (2, 0), (1, 1), (1, 0), (3, 1), (3, 0), (0, 1)):
        pltpu.make_async_remote_copy(
            src_ref=flag, dst_ref=flags.at[mine], send_sem=sendf, recv_sem=gotf,
            device_id=(cut_of[dx][dc], stem_of[0][0]), device_id_type=MESH,
        ).start()
    halves_of = [px // 2 for px in xs]
    cols = [[4 * pc + 2 * (px - 2 * half) + 1 for pc in cs] for px, half in zip(xs, halves_of)]
    rows_of = [lax.rem(py + 2, 8) * 8 for py in ys]
    flips = [lax.rem(py + 6, 8) * 8 - row for py, row in zip(ys, rows_of)]
    for dx, dy, dc, dz in mates:
        theirs = rows_of[dy] + halves_of[dx] * flips[dy] + cols[dx][dc] - zs[dz]
        pltpu.make_async_remote_copy(
            src_ref=sendbuf.at[theirs], dst_ref=recv1.at[slot], send_sem=send1, recv_sem=got1.at[dx],
            device_id=(cut_of[dx][dc], stem_of[dy][dz]), device_id_type=MESH,
        ).start()
    for pzh, pzp, there_z in source_z:

        @pl.when(there_z < height)
        def _(pzh=pzh, pzp=pzp):
            for pyh in range(2):
                there = (pzh * 8 + qx * 2 + qc, pyh * 32 + qy * 8 + pzp * 2 + qz)
                pl.semaphore_signal(ready.at[zh], inc=1, device_id=there, device_id_type=MESH)

    recv1[slot] = sendbuf[group]
    flags[mine] = flag[...]

    loads[3].wait()
    sub = iota((128, 512), 0)
    source = (((sub // 32) * 8 + zp * 2 + (sub // 16) % 2) * 2 + (sub // 8) % 2) * 8 + sub % 8
    pick2 = one_hot(source, spread(wide, perms, 2))
    column = iota((256, 256), 1)
    owner = jnp.zeros((1, 256), jnp.int32)
    block_of = iota((1, 256), 1) // 16
    for b in range(16):
        owner = jnp.where(block_of == b, owners[b], owner)
    deal = one_hot(iota((256, 256), 0), owner * 16 + iota((1, 256), 1) % 16)
    both = []
    for v in range(2):
        parts = [mm(mm(pick2, clv[v, q]).astype(BF), deal) for q in range(2)]
        both.append(jnp.concatenate(parts, axis=1).T)
    pltpu.make_async_copy(flags.at[pl.ds(0, 7)], flags.at[pl.ds(0, 7)], gotf).wait()
    for c in range(8):
        on = jnp.broadcast_to(flags[c][:1], (512, 128)) > 0.5
        w3[c // 2, :, (c % 2) * 128:(c % 2) * 128 + 128] = jnp.where(on, both[1], both[0]).astype(BF)

    f = None
    for dx in (2, 1, 3, 0):
        px = xs[(4 - dx) % 4]
        came = recv1.at[pl.ds(px * 16, 16 if dx else 15)]
        pltpu.make_async_copy(came, came, got1.at[dx]).wait()
        term = mm(w3[px], recv1[pl.ds(px * 16, 16)].reshape(256, 128))
        f = term if f is None else f + term
    fbuf[...] = fold(f[:256], f[256:], even).reshape(16, 16, 128).astype(BF)

    pool = zh * 8 + yh * 4 + zp

    for pzh in range(2):

        @pl.when(owner_z[pzh] > height)
        def _(pzh=pzh):
            pl.semaphore_wait(ready.at[pzh], 8)

        for dx in (2, 1, 3, 0):
            for dc in (1, 0):
                b = pzh * 8 + xs[dx] * 2 + cs[dc]
                pltpu.make_async_remote_copy(
                    src_ref=fbuf.at[b], dst_ref=recv2.at[pool], send_sem=send2, recv_sem=got2,
                    device_id=(b, group), device_id_type=MESH,
                ).start()
    pltpu.make_async_copy(recv2, recv2, got2).wait()
    sums = []
    for h in range(2):
        total = jnp.zeros((16, 128), F32)
        for z2 in range(2):
            for k in range(4):
                total = total + recv2[z2 * 8 + h * 4 + k].astype(F32)
        sums.append(total)
    out_ref[0] = jnp.where(even, sums[0], turn(sums[1], 1))
    out_ref[1] = jnp.where(even, turn(sums[0], -1), sums[1])

    pltpu.make_async_copy(flags.at[pl.ds(0, 7)], flags.at[pl.ds(0, 7)], sendf).wait()
    pltpu.make_async_copy(sendbuf.at[pl.ds(0, 63)], sendbuf.at[pl.ds(0, 63)], send1).wait()
    pltpu.make_async_copy(fbuf, fbuf, send2).wait()


def body(stems, branches, closing, slice_values, mode_perms, owner_map):
    hbm = pl.BlockSpec(memory_space=pl.ANY)
    out = pl.pallas_call(
        kernel,
        out_shape=pltpu.VMEM((2, 16, 128), F32),
        in_specs=[hbm] * 6,
        out_specs=pl.BlockSpec(memory_space=pltpu.VMEM),
        scratch_shapes=[
            pltpu.VMEM((128, 2, 512), BF),
            pltpu.VMEM((2, 2, 512, 512), BF),
            pltpu.VMEM((2, 2, 512, 512), BF),
            pltpu.VMEM((2, 2, 512, 256), BF),
            pltpu.VMEM((64, 16, 128), BF),
            pltpu.VMEM((64, 16, 128), BF),
            pltpu.VMEM((16, 16, 128), BF),
            pltpu.VMEM((16, 16, 128), BF),
            pltpu.VMEM((8, 128), F32),
            pltpu.VMEM((8, 8, 128), F32),
            pltpu.VMEM((4, 512, 256), BF),
            pltpu.SMEM((1, 3), jnp.int32),
            pltpu.SMEM((3, 9), jnp.int32),
            pltpu.SMEM((16,), jnp.int32),
            pltpu.SemaphoreType.DMA((7,)),
            pltpu.SemaphoreType.DMA,
            pltpu.SemaphoreType.DMA((4,)),
            pltpu.SemaphoreType.DMA,
            pltpu.SemaphoreType.DMA,
            pltpu.SemaphoreType.DMA,
            pltpu.SemaphoreType.DMA,
            pltpu.SemaphoreType.REGULAR((2,)),
        ],
        compiler_params=pltpu.CompilerParams(collective_id=0, has_side_effects=True),
    )(slice_values, mode_perms, owner_map, stems.reshape(128, 2, 512), branches, closing)
    return out.reshape(1, 1, 2, 16, 128)


def solution(mesh):
    in_specs = (P("cuts", "stem", None, None, None), P(), P(), P("cuts", None), P(), P())
    out_specs = P("stem", "cuts", None, None, None)
    return jax.shard_map(body, mesh=mesh, in_specs=in_specs, out_specs=out_specs, check_vma=False)
```
